32 devices in a mesh: gx: 4 (over z), gy: 8 (over y, x, core).
Axes of the slice: x: 2, y: 2, z: 4, core: 2. Of those that a mesh axis runs over, the one named last changes fastest.
Arguments:
- splats: float32 [1024, 55, 128], P(('gx', 'gy')), as said below
- moment_one: float32 [1024, 55, 128], P(('gx', 'gy')), may hold values from -0.3 to 0.3
- moment_two: float32 [1024, 55, 128], P(('gx', 'gy')), may hold values from 0.001 to 1
- target: float32 [512, 3, 256], P(('gx', 'gy')), may hold values from 0 to 1
- tile_place: int32 [512], P(('gx', 'gy')), may hold values from 0 to 511, as said below
- pairs: int32 [512, 8], P(('gx', 'gy')), may hold values from -1 to 63, as said below
- fetch: int32 [32, 32, 2], P(('gx', 'gy')), may hold values from -1 to 31, as said below
Outputs:
- image: float32 [512, 3, 256], P(('gx', 'gy'))
- splat_grad: float32 [1024, 55, 128], P(('gx', 'gy'))
- adam_step: float32 [1024, 55, 128], P(('gx', 'gy'))
The draws below stay inside these ranges and needn't reach their ends.
Inputs may be any that keep to these rules, and one draw needn't show every extreme that they name: fetch[d, o] lists up to 2 distinct blocks of owner o (indices among the owner's 32 blocks, owner o holding global blocks o * 32 to o * 32 + 31) that device d fetches; -1 marks an empty place; every device fetches 2 blocks from some owner. pairs[r] names distinct fetched places s = o * 2 + i of the device that holds row r, each with fetch[that device, o, i] >= 0; -1 marks empty places, which come last; on every device some row has all 8 places live. `tile_place`: a permutation of the view tiles; view tiles are numbered row by row, 16 to a row. z = splats[:, 2] lies between 2 and 12.
All inputs are finite; a program needn't handle non-finite values.
Results may differ from the reference program's by a relative error of at most 0.0003.
Values sent between devices are 32-bit elements; how exact they have to be, the bound alone decides.
A program may use at most 128 MiB of HBM per device.

```python
import math
import jax
import jax.numpy as jnp
from jax import lax

NP = 55
BS = 128
CAP = 2
DEPTH = 8
TILES_DEV = 16
TX = 16
BLK_DEV = 32
BLOCKS = 1024
TILES = 512
N_GX = 4
N_GY = 8


def layout(key):
    devices = N_GX * N_GY
    classes = TILES_DEV
    members = devices // TILES_DEV
    band_rows = devices // TX
    slots = devices * CAP
    keys = jax.random.split(jax.random.fold_in(key, 7), 6)
    index = jnp.arange(devices, dtype=jnp.int32)
    band_index = jnp.arange(classes, dtype=jnp.int32)
    corner_score = jax.random.randint(keys[0], (classes, devices), 0, 1 << 16) * devices + index[None, :]
    corner_owner = jnp.argsort(corner_score, axis=1).astype(jnp.int32)
    owner_corner = jnp.argsort(corner_owner, axis=1).astype(jnp.int32)
    local_score = jax.random.randint(keys[1], (devices, BLK_DEV), 0, 1 << 16) * BLK_DEV + jnp.arange(BLK_DEV, dtype=jnp.int32)[None, :]
    local_order = jnp.argsort(local_score, axis=1).astype(jnp.int32)
    local_rank = jnp.argsort(local_order, axis=1).astype(jnp.int32)
    tile_row = index // TX
    tile_col = index % TX
    inner = (tile_row >= 1) & (tile_col >= 1)
    first_score = jax.random.randint(keys[2], (classes, devices), 0, 1 << 16) * devices + index[None, :] + jnp.where(inner, 0, 1 << 24)[None, :]
    first_rank = jnp.argsort(jnp.argsort(first_score, axis=1), axis=1)
    later = jax.random.randint(keys[3], (classes, devices), 0, 1 << 16) * devices + index[None, :]
    second_score = jnp.where(first_rank < members, first_rank, members + later)
    order = jnp.argsort(second_score, axis=1).astype(jnp.int32)
    group_member = jnp.arange(members, dtype=jnp.int32)
    turn = jnp.arange(TILES_DEV, dtype=jnp.int32)
    position = jnp.where(turn[None, :] == 0, group_member[:, None], members + group_member[:, None] * (TILES_DEV - 1) + turn[None, :] - 1).reshape(-1)
    band_tiles = order[:, position]
    tile_place = (band_index[:, None] * devices + band_tiles).reshape(-1).astype(jnp.int32)
    corner_table = jnp.stack([jnp.where(inner, (tile_row - 1) * TX + tile_col - 1, -1), jnp.where(tile_row >= 1, (tile_row - 1) * TX + tile_col, -1), jnp.where(tile_col >= 1, tile_row * TX + tile_col - 1, -1), index], axis=1)
    first_corners = corner_table[order[:, :members]].reshape(classes, members * 4)
    hit_first = jnp.any(first_corners[:, :, None] == index[None, None, :], axis=1)
    full = (jax.random.randint(keys[4], (classes, devices), 0, 100) < 80) | hit_first
    live_block = (jnp.arange(CAP)[None, None, :] == 0) | full[:, :, None]
    row_corners = corner_table[band_tiles]
    device_corners = row_corners.reshape(classes, members, TILES_DEV * 4)
    need = jnp.any(device_corners[:, :, :, None] == index[None, None, None, :], axis=2)
    need_owner = jnp.take_along_axis(need, jnp.broadcast_to(owner_corner[:, None, :], need.shape), axis=2)
    live_owner = jnp.take_along_axis(live_block, jnp.broadcast_to(owner_corner[:, :, None], (classes, devices, CAP)), axis=1)
    chosen = local_order[index[None, :, None], band_index[:, None, None] * CAP + jnp.arange(CAP, dtype=jnp.int32)[None, None, :]]
    fetch = jnp.where(need_owner[:, :, :, None] & live_owner[:, None, :, :], chosen[:, None, :, :], -1)
    fetch = fetch.reshape(devices, devices, CAP).astype(jnp.int32)
    valid = row_corners >= 0
    safe = jnp.maximum(row_corners, 0)
    entry = (safe[:, :, :, None] * CAP + jnp.arange(CAP)[None, None, None, :]).reshape(classes, devices * 4 * CAP)
    entry_live = jnp.take_along_axis(live_block.reshape(classes, slots), entry, axis=1).reshape(classes, devices, 4 * CAP)
    entry_live = entry_live & jnp.repeat(valid, CAP, axis=2)
    owners = jnp.take_along_axis(corner_owner, safe.reshape(classes, -1), axis=1).reshape(classes, devices, 4)
    places = (owners[:, :, :, None] * CAP + jnp.arange(CAP)[None, None, None, :]).reshape(classes, devices, 4 * CAP)
    depth_key = jax.random.randint(keys[5], (classes, slots), 0, 1 << 12) * slots + jnp.arange(slots)[None, :]
    entry_sort_key = jnp.take_along_axis(depth_key, entry, axis=1).reshape(classes, devices, 4 * CAP)
    spare = jnp.arange(4 * CAP)[None, None, :]
    score = jnp.where(entry_live, (1 << 30) - entry_sort_key, -1 - spare)
    best, taken = lax.top_k(score, DEPTH)
    picked = jnp.take_along_axis(places, taken, axis=2)
    pairs = jnp.where(best >= 0, picked, -1).reshape(TILES, DEPTH).astype(jnp.int32)
    block_owner = jnp.repeat(index, BLK_DEV)
    block_local = jnp.tile(jnp.arange(BLK_DEV, dtype=jnp.int32), devices)
    rank = local_rank[block_owner, block_local]
    band = rank // CAP
    which = rank % CAP
    corner = owner_corner[band, block_owner]
    centre_x = (16 * (corner % TX + 1)).astype(jnp.float32)
    centre_y = (16 * (band * band_rows + corner // TX + 1)).astype(jnp.float32)
    near = 2.0 + 9.0 * depth_key[band, corner * CAP + which].astype(jnp.float32) / float((1 << 12) * slots)
    return (fetch, pairs, tile_place, centre_x, centre_y, near)


def draw_fetch(key, part):
    return layout(key)[0]


def draw_pairs(key, part):
    return layout(key)[1]


def draw_tile_place(key, part):
    return layout(key)[2]


def draw_splats(key, part):
    _, _, _, centre_x, centre_y, near = layout(key)
    keys = jax.random.split(jax.random.fold_in(key, 11), 8)
    shape = (BLOCKS, BS)
    width = 16.0 * TX
    height = 16.0 * (TILES // TX)
    harmonic_scale = jnp.where(jnp.arange(48) % 16 == 0, 0.6, 0.2)[None, :, None]
    power_draw = jax.random.uniform(keys[3], shape, jnp.float32)
    spread = 4.0
    lower, upper = (3.5, 11.0)
    logit = -8.0 + 9.0 * power_draw ** 20
    jitter = 0.9
    coeffs = jax.random.normal(keys[4], (BLOCKS, 48, BS), jnp.float32) * harmonic_scale
    across = centre_x[:, None] + jax.random.uniform(keys[0], shape, jnp.float32, -spread, spread)
    down = centre_y[:, None] + jax.random.uniform(keys[1], shape, jnp.float32, -spread, spread)
    depth = near[:, None] + jax.random.uniform(keys[2], shape, jnp.float32, 0.0, jitter)
    first_scale = jax.random.uniform(keys[5], shape, jnp.float32, math.log(lower), math.log(upper))
    second_scale = jax.random.uniform(keys[6], shape, jnp.float32, math.log(lower), math.log(upper))
    angle = jax.random.uniform(keys[7], shape, jnp.float32, -math.pi, math.pi)
    place_x = (across - 0.5 * width) * depth / width
    place_y = (down - 0.5 * height) * depth / width
    head = jnp.stack([place_x, place_y, depth, first_scale, second_scale, angle, logit], axis=1)
    return jnp.concatenate([head, coeffs], axis=1).astype(jnp.float32)


def levels(key, dims, cuts, least, high):
    factor_of = 1.0
    for dim, parts in cuts:
        heights = jax.random.uniform(jax.random.fold_in(jax.random.fold_in(key, 6), dim), (parts,), jnp.float32, least / len(cuts), high / len(cuts))
        factor_of = factor_of * jnp.repeat(jnp.exp(heights), dims[dim] // parts).reshape((-1,) + (1,) * (len(dims) - 1 - dim))
    return factor_of


def noise(own_key, shape, scale, limit, cuts=(), held_as=jnp.bfloat16):
    result = jax.random.normal(own_key, shape, jnp.float32) * scale
    if len(cuts) > 0:
        result = levels(own_key, shape, cuts, -0.22, 0.18) * result
    return jnp.clip(result, min=-limit, max=limit).astype(held_as)


def setup_inputs(seed: int = 0) -> dict:
    streams_of = jax.random.split(jax.random.key(seed), 8)
    splats = draw_splats(jax.random.fold_in(streams_of[7], 71), 0)
    moment_one = noise(streams_of[1], (BLOCKS, NP, BS), 0.05, 0.3, ((0, 32),), jnp.float32)
    moment_two = jnp.clip(jnp.exp(math.log(1.0) - 6.9077552 * jax.random.uniform(streams_of[2], (BLOCKS, NP, BS), jnp.float32) ** levels(streams_of[2], (BLOCKS, NP, BS), ((0, 32),), -0.2, 0.2)), 0.001, 1.0)
    target = jnp.clip(1.0 * jax.random.uniform(streams_of[3], (TILES, 3, 256), jnp.float32) ** levels(streams_of[3], (TILES, 3, 256), ((0, 32),), -0.2, 0.2), 0.0, 1.0)
    tile_place = draw_tile_place(jax.random.fold_in(streams_of[7], 71), 0)
    pairs = draw_pairs(jax.random.fold_in(streams_of[7], 71), 0)
    fetch = draw_fetch(jax.random.fold_in(streams_of[7], 71), 0)
    return dict(splats=splats, moment_one=moment_one, moment_two=moment_two, target=target, tile_place=tile_place, pairs=pairs, fetch=fetch)


HARMONIC_ZERO = 0.28209479177387814
HARMONIC_ONE = 0.4886025119029199
HARMONIC_TWO = (1.0925484305920792, -1.0925484305920792, 0.31539156525252005, -1.0925484305920792, 0.5462742152960396)
HARMONIC_THREE = (-0.5900435899266435, 2.890611442640554, -0.4570457994644658, 0.3731763325901154, -0.4570457994644658, 1.445305721320277, -0.5900435899266435)

def harmonics(east, north, ahead):
    east_east = east * east
    north_north = north * north
    ahead_ahead = ahead * ahead
    terms = [jnp.full_like(east, HARMONIC_ZERO), -HARMONIC_ONE * north, HARMONIC_ONE * ahead, -HARMONIC_ONE * east, HARMONIC_TWO[0] * east * north, HARMONIC_TWO[1] * north * ahead, HARMONIC_TWO[2] * (2.0 * ahead_ahead - east_east - north_north), HARMONIC_TWO[3] * east * ahead, HARMONIC_TWO[4] * (east_east - north_north), HARMONIC_THREE[0] * north * (3.0 * east_east - north_north), HARMONIC_THREE[1] * east * north * ahead, HARMONIC_THREE[2] * north * (4.0 * ahead_ahead - east_east - north_north), HARMONIC_THREE[3] * ahead * (2.0 * ahead_ahead - 3.0 * east_east - 3.0 * north_north), HARMONIC_THREE[4] * east * (4.0 * ahead_ahead - east_east - north_north), HARMONIC_THREE[5] * ahead * (east_east - north_north), HARMONIC_THREE[6] * east * (east_east - 3.0 * north_north)]
    return jnp.stack(terms, axis=1)

def derive(raw, width, height):
    place_x = raw[:, 0]
    place_y = raw[:, 1]
    place_z = raw[:, 2]
    screen_u = width * place_x / place_z + 0.5 * width
    screen_v = width * place_y / place_z + 0.5 * height
    inverse_one = jnp.exp(-2.0 * raw[:, 3])
    inverse_two = jnp.exp(-2.0 * raw[:, 4])
    cosine = jnp.cos(raw[:, 5])
    sine = jnp.sin(raw[:, 5])
    conic_a = cosine * cosine * inverse_one + sine * sine * inverse_two
    conic_b = cosine * sine * (inverse_one - inverse_two)
    conic_c = sine * sine * inverse_one + cosine * cosine * inverse_two
    opacity = jax.nn.sigmoid(raw[:, 6])
    length = jnp.sqrt(place_x * place_x + place_y * place_y + place_z * place_z)
    basis = harmonics(place_x / length, place_y / length, place_z / length)
    coeffs = raw[:, 7:].reshape(raw.shape[0], 3, 16, raw.shape[2])
    colors = 0.5 + lax.optimization_barrier(jnp.sum(coeffs * basis[:, None], axis=2))
    head = jnp.stack([screen_u, screen_v, conic_a, conic_b, conic_c, opacity], axis=1)
    return jnp.concatenate([head, colors], axis=1)

def composite(screens, pixel_x, pixel_y):

    def advance(carry, screen_splat):
        log_trans, pixel_colour = carry
        delta_x = pixel_x[:, :, None] - screen_splat[:, None, 0]
        delta_y = pixel_y[:, :, None] - screen_splat[:, None, 1]
        power = -0.5 * (screen_splat[:, None, 2] * delta_x * delta_x + 2.0 * screen_splat[:, None, 3] * delta_x * delta_y + screen_splat[:, None, 4] * delta_y * delta_y)
        alpha = screen_splat[:, None, 5] * jnp.exp(power)
        log_keep = jnp.log1p(-alpha)
        before = jnp.cumsum(log_keep, axis=2) - log_keep
        blend_weight = alpha * jnp.exp(log_trans[:, :, None] + before)
        pixel_colour = pixel_colour + jnp.einsum('ylo,yeo->yel', blend_weight, screen_splat[:, 6:9], precision=lax.Precision.HIGHEST)
        return ((log_trans + lax.optimization_barrier(jnp.sum(log_keep, axis=2)), pixel_colour), None)
    count = screens.shape[0]
    start = (jnp.zeros((count, 256), jnp.float32), jnp.zeros((count, 3, 256), jnp.float32))
    (_, pixel_colour), _ = lax.scan(jax.checkpoint(advance), start, jnp.moveaxis(screens, 1, 0))
    return pixel_colour

def reference(splats, moment_one, moment_two, target, tile_place, pairs, fetch):
    devices = N_GX * N_GY
    width = 16.0 * TX
    height = 16.0 * (TILES // TX)
    screen_all, pull_all = jax.vjp(lambda raw: derive(raw, width, height), splats)
    rows = jnp.arange(TILES, dtype=jnp.int32)
    device_of = rows // TILES_DEV
    place = jnp.maximum(pairs, 0).astype(jnp.int32)
    flat_index = (device_of[:, None] * (devices * CAP) + place).astype(jnp.int32)
    local = fetch.reshape(-1)[flat_index]
    block_id = jnp.where(pairs >= 0, place // CAP * BLK_DEV + local, 0).astype(jnp.int32)
    used = (pairs >= 0).astype(jnp.float32)
    pixel = jnp.arange(256, dtype=jnp.int32)
    corner_x = (tile_place % TX * 16).astype(jnp.float32)
    corner_y = (tile_place // TX * 16).astype(jnp.float32)
    pixel_x = corner_x[:, None] + (pixel % 16).astype(jnp.float32)[None, :] + 0.5
    pixel_y = corner_y[:, None] + (pixel // 16).astype(jnp.float32)[None, :] + 0.5
    group = 16
    groups = TILES // group

    def one_group(total, pieces):
        ids, mask, across, down, goal = pieces
        slots = screen_all[ids] * mask[:, :, None, None]

        def objective(screens):
            image = composite(screens, across, down)
            residual = image - goal
            return (image, jnp.sum(residual * residual) / 512.0)
        (image, loss), pull = jax.vjp(objective, slots)
        grads, = pull((jnp.zeros_like(image), jnp.ones_like(loss)))
        grads = grads * mask[:, :, None, None]
        total = total.at[ids.reshape(-1)].add(grads.reshape((-1,) + grads.shape[2:]))
        return (total, image)
    pieces = (block_id.reshape(groups, group, DEPTH), used.reshape(groups, group, DEPTH), pixel_x.reshape(groups, group, 256), pixel_y.reshape(groups, group, 256), target.reshape(groups, group, 3, 256))
    total, images = lax.scan(one_group, jnp.zeros_like(screen_all), pieces)
    image = images.reshape(TILES, 3, 256)
    splat_grad, = pull_all(total)
    first = 0.9 * moment_one + 0.1 * splat_grad
    second_moment = 0.999 * moment_two + 0.001 * splat_grad * splat_grad
    adam_step = first / (jnp.sqrt(second_moment) + 1e-08)
    return (image, splat_grad, adam_step)
```

```python
import functools

import jax
import jax.numpy as jnp
import numpy as np
from jax import lax
from jax.experimental import pallas as pl
from jax.experimental.pallas import tpu as pltpu
from jax.sharding import PartitionSpec as P

TX = 16
SIDE = 16
PIXELS = SIDE * SIDE
LOG2E = 1.4426950408889634
DEAD = -1.0e4
GROUP = 2
F32 = jnp.float32
BF16 = jnp.bfloat16


HARMONIC_ZERO = 0.28209479177387814
HARMONIC_ONE = 0.4886025119029199
HARMONIC_TWO = (
    1.0925484305920792,
    -1.0925484305920792,
    0.31539156525252005,
    -1.0925484305920792,
    0.5462742152960396,
)
HARMONIC_THREE = (
    -0.5900435899266435,
    2.890611442640554,
    -0.4570457994644658,
    0.3731763325901154,
    -0.4570457994644658,
    1.445305721320277,
    -0.5900435899266435,
)


def harmonics(east, north, ahead):
    east_east = east * east
    north_north = north * north
    ahead_ahead = ahead * ahead
    terms = [
        jnp.full_like(east, HARMONIC_ZERO),
        -HARMONIC_ONE * north,
        HARMONIC_ONE * ahead,
        -HARMONIC_ONE * east,
        HARMONIC_TWO[0] * east * north,
        HARMONIC_TWO[1] * north * ahead,
        HARMONIC_TWO[2] * (2.0 * ahead_ahead - east_east - north_north),
        HARMONIC_TWO[3] * east * ahead,
        HARMONIC_TWO[4] * (east_east - north_north),
        HARMONIC_THREE[0] * north * (3.0 * east_east - north_north),
        HARMONIC_THREE[1] * east * north * ahead,
        HARMONIC_THREE[2] * north * (4.0 * ahead_ahead - east_east - north_north),
        HARMONIC_THREE[3] * ahead * (2.0 * ahead_ahead - 3.0 * east_east - 3.0 * north_north),
        HARMONIC_THREE[4] * east * (4.0 * ahead_ahead - east_east - north_north),
        HARMONIC_THREE[5] * ahead * (east_east - north_north),
        HARMONIC_THREE[6] * east * (east_east - 3.0 * north_north),
    ]
    return jnp.stack(terms, axis=1)


def derive(raw, width, height):
    place_x = raw[:, 0]
    place_y = raw[:, 1]
    place_z = raw[:, 2]
    screen_u = width * place_x / place_z + 0.5 * width
    screen_v = width * place_y / place_z + 0.5 * height
    inverse_one = jnp.exp(-2.0 * raw[:, 3])
    inverse_two = jnp.exp(-2.0 * raw[:, 4])
    cosine = jnp.cos(raw[:, 5])
    sine = jnp.sin(raw[:, 5])
    conic_a = cosine * cosine * inverse_one + sine * sine * inverse_two
    conic_b = cosine * sine * (inverse_one - inverse_two)
    conic_c = sine * sine * inverse_one + cosine * cosine * inverse_two
    log_opacity = jax.nn.log_sigmoid(raw[:, 6])
    length = jnp.sqrt(place_x * place_x + place_y * place_y + place_z * place_z)
    basis = harmonics(place_x / length, place_y / length, place_z / length)
    coeffs = raw[:, 7:].reshape(raw.shape[0], 3, 16, raw.shape[2])
    colors = 0.5 + jnp.sum(coeffs * basis[:, None], axis=2)
    head = jnp.stack([screen_u, screen_v, conic_a, conic_b, conic_c, log_opacity], axis=1)
    return jnp.concatenate([head, colors], axis=1)


def pixel_basis():
    j = np.arange(PIXELS)
    x = j % SIDE + 0.5 - SIDE / 2
    y = j // SIDE + 0.5 - SIDE / 2
    rows = np.stack([x * x, x * y, y * y, x, y, np.ones_like(x), 0 * x, 0 * x])
    return np.concatenate([rows, rows, rows, 0 * rows]).astype(np.float32)


def lane_order(block):
    row = np.arange(block)
    splat = (row % 8) * (block // 8) + row // 8
    return (np.arange(block)[:, None] == splat[None, :]).astype(np.float32)


def rounded(x):
    return x.astype(BF16).astype(F32)


def shifted(x, shift):
    return pltpu.roll(x, shift % 8, 0)


def blend_kernel(
    pairs_ref, place_ref, basis_ref, arrived_ref, target_ref, image_ref, grad_ref,
    screen, coef, colour, alphas, weights, halves, products, steps, resid, moments, grads,
):
    step = pl.program_id(0)
    depth = pairs_ref.shape[1]
    block = arrived_ref.shape[2]
    chunks = block // 8
    sub = lax.broadcasted_iota(jnp.int32, (8, PIXELS), 0)
    sub_lane = lax.broadcasted_iota(jnp.int32, (8, block), 0)

    @pl.when(step == 0)
    def _():
        grad_ref[...] = jnp.zeros_like(grad_ref)
        coef[...] = jnp.zeros_like(coef)
        colour[...] = jnp.zeros_like(colour)
        resid[...] = jnp.zeros_like(resid)

    live = []
    centre = []
    deepest = jnp.int32(0)
    for t in range(GROUP):
        row = step * GROUP + t
        tile = place_ref[row]
        count = jnp.int32(0)
        for k in range(depth):
            slot = pairs_ref[row, k]
            count = count + (slot >= 0).astype(jnp.int32)
            screen[t, 0:9, k, :] = arrived_ref[jnp.maximum(slot, 0)]
        live.append(count)
        deepest = jnp.maximum(deepest, count)
        cx = (lax.rem(tile, TX) * SIDE + SIDE // 2).astype(F32)
        cy = (lax.div(tile, TX) * SIDE + SIDE // 2).astype(F32)
        centre.append((cx, cy))
        u = screen[t, 0] - cx
        v = screen[t, 1] - cy
        a, b, c = screen[t, 2], screen[t, 3], screen[t, 4]
        opac = jnp.maximum(screen[t, 5], DEAD)
        lin_x = a * u + b * v
        lin_y = b * u + c * v
        const = opac - 0.5 * (lin_x * u + lin_y * v)
        on = sub_lane < count
        for j, value in enumerate((-0.5 * a, -b, -0.5 * c, lin_x, lin_y, const)):
            coef[t, j] = jnp.where(on, LOG2E * value, DEAD if j == 5 else 0.0)
        for h in range(3):
            colour[t, h] = screen[t, 6 + h]

    basis = basis_ref[...].astype(BF16)
    zero8 = jnp.zeros((8, block), F32)
    zero_row = jnp.zeros((8, PIXELS), F32)

    def forward(k, carry):
        after = []
        for t in range(GROUP):
            trans, total = carry[2 * t], carry[2 * t + 1]
            c = coef[t, :, k, :]
            c1 = rounded(c)
            c2 = rounded(c - c1)
            c3 = c - c1 - c2
            parts = jnp.concatenate([c1, c2, c3, zero8], axis=0).astype(BF16)
            power = lax.dot_general(
                parts, basis, (((0,), (0,)), ((), ())), preferred_element_type=F32
            )
            alpha = jnp.exp2(power)
            alphas[t, k] = alpha
            keep = 1.0 - alpha
            kept = keep[0:8]
            for i in range(1, chunks):
                kept = kept * keep[8 * i : 8 * i + 8]
            products[t, k] = kept
            scan = jnp.where(sub == 0, trans, shifted(kept, 1))
            for d in (1, 2, 4):
                scan = scan * jnp.where(sub < d, 1.0, shifted(scan, d))
            trans = jnp.broadcast_to((scan * kept)[7:8], (8, PIXELS))
            here = scan
            for i in range(0, chunks, 2):
                one = alpha[8 * i : 8 * i + 8] * here
                here = here * keep[8 * i : 8 * i + 8]
                two = alpha[8 * i + 8 : 8 * i + 16] * here
                here = here * keep[8 * i + 8 : 8 * i + 16]
                pair = jnp.concatenate([one, two], axis=0)
                weights[t, k, 8 * i : 8 * i + 16] = pair
                high = pair.astype(BF16)
                halves[t, k, 8 * i : 8 * i + 16] = high
                halves[t, k, block + 8 * i : block + 8 * i + 16] = (
                    pair - high.astype(F32)
                ).astype(BF16)
            hue = colour[t, :, k, :]
            hue1 = rounded(hue)
            hue2 = hue - hue1
            left = jnp.concatenate(
                [
                    jnp.concatenate([hue1, hue1], axis=1),
                    jnp.concatenate([hue2, zero8], axis=1),
                ],
                axis=0,
            ).astype(BF16)
            total = total + jnp.dot(left, halves[t, k], preferred_element_type=F32)
            after += [trans, total]
        return tuple(after)

    start = (jnp.ones((8, PIXELS), F32), jnp.zeros((16, PIXELS), F32)) * GROUP
    done = lax.fori_loop(0, deepest, forward, start)

    slopes = []
    for t in range(GROUP):
        total = done[2 * t + 1]
        image = (total[0:8] + total[8:16])[0:3]
        image_ref[t] = image
        resid[t, 0:3] = (image - target_ref[t]) * (2.0 / 512.0)
        g = resid[t]
        g1 = rounded(g)
        g2 = g - g1
        slopes.append(
            (
                jnp.concatenate([g1, g1, g2, zero_row], axis=0).astype(BF16),
                jnp.concatenate([g1, g2], axis=0).astype(BF16),
            )
        )
    monomials = basis_ref[0:16].astype(BF16)

    def backward(index, carry):
        k = deepest - 1 - index
        after = []
        for t in range(GROUP):
            behind = carry[t]
            g3, g2 = slopes[t]
            hue = colour[t, :, k, :]
            hue1 = rounded(hue)
            hue2 = hue - hue1
            left = jnp.concatenate([hue1, hue2, hue1, zero8], axis=0).astype(BF16)
            slope = lax.dot_general(
                left, g3, (((0,), (0,)), ((), ())), preferred_element_type=F32
            )
            alpha = alphas[t, k]
            keep = 1.0 - alpha
            lit = alpha * slope
            gather = lit[block - 8 : block]
            for i in range(chunks - 2, -1, -1):
                gather = lit[8 * i : 8 * i + 8] + keep[8 * i : 8 * i + 8] * gather
            kept = products[t, k]
            scan = jnp.where(sub == 7, behind, shifted(gather, -1))
            rate = jnp.where(sub == 7, 0.0, shifted(kept, -1))
            for d in (1, 2, 4):
                inside = sub < 8 - d
                scan = scan + rate * jnp.where(inside, shifted(scan, -d), 0.0)
                rate = rate * jnp.where(inside, shifted(rate, -d), 1.0)
            after.append(jnp.broadcast_to((gather + kept * scan)[0:1], (8, PIXELS)))
            here = scan
            for i in range(chunks - 2, -1, -2):
                lo, mid, hi = 8 * i, 8 * i + 8, 8 * i + 16
                two = weights[t, k, mid:hi] * (slope[mid:hi] - here)
                here = lit[mid:hi] + keep[mid:hi] * here
                one = weights[t, k, lo:mid] * (slope[lo:mid] - here)
                here = lit[lo:mid] + keep[lo:mid] * here
                pair = jnp.concatenate([one, two], axis=0)
                high = pair.astype(BF16)
                steps[t, lo:hi] = high
                steps[t, block + lo : block + hi] = (pair - high.astype(F32)).astype(BF16)
            sums = lax.dot_general(
                monomials, steps[t], (((1,), (1,)), ((), ())), preferred_element_type=F32
            )
            moments[t, 0:8, k, :] = sums[0:8, 0:block] + sums[0:8, block:]
            hues = lax.dot_general(
                g2, halves[t, k], (((1,), (1,)), ((), ())), preferred_element_type=F32
            )
            moments[t, 8:16, k, :] = hues[0:8, 0:block] + hues[0:8, block:] + hues[8:16, 0:block]
        return tuple(after)

    lax.fori_loop(0, deepest, backward, (jnp.zeros((8, PIXELS), F32),) * GROUP)

    for t in range(GROUP):
        row = step * GROUP + t
        cx, cy = centre[t]
        u = screen[t, 0] - cx
        v = screen[t, 1] - cy
        a, b, c = screen[t, 2], screen[t, 3], screen[t, 4]
        mxx, mxy, myy = moments[t, 0], moments[t, 1], moments[t, 2]
        mx, my, m = moments[t, 3], moments[t, 4], moments[t, 5]
        off_x = mx - u * m
        off_y = my - v * m
        grads[t, 0] = a * off_x + b * off_y
        grads[t, 1] = b * off_x + c * off_y
        grads[t, 2] = -0.5 * (mxx - u * (mx + off_x))
        grads[t, 3] = -(mxy - u * my - v * off_x)
        grads[t, 4] = -0.5 * (myy - v * (my + off_y))
        grads[t, 5] = m
        for h in range(3):
            grads[t, 6 + h] = moments[t, 8 + h]
        for k in range(depth):

            @pl.when(k < live[t])
            def _():
                slot = pairs_ref[row, k]
                grad_ref[slot] = grad_ref[slot] + grads[t, 0:9, k, :]


def blend(arrived, target, tile_place, pairs):
    tiles, channels, pixels = target.shape
    depth = pairs.shape[1]
    slots, rows, block = arrived.shape
    basis = jnp.asarray(pixel_basis())
    whole = lambda s, *_: (0, 0, 0)
    return pl.pallas_call(
        blend_kernel,
        grid_spec=pltpu.PrefetchScalarGridSpec(
            num_scalar_prefetch=2,
            grid=(tiles // GROUP,),
            in_specs=[
                pl.BlockSpec(basis.shape, lambda s, *_: (0, 0)),
                pl.BlockSpec(arrived.shape, whole),
                pl.BlockSpec((GROUP, channels, pixels), lambda s, *_: (s, 0, 0)),
            ],
            out_specs=[
                pl.BlockSpec((GROUP, channels, pixels), lambda s, *_: (s, 0, 0)),
                pl.BlockSpec(arrived.shape, whole),
            ],
            scratch_shapes=[
                pltpu.VMEM((GROUP, 16, depth, block), F32),
                pltpu.VMEM((GROUP, 8, depth, block), F32),
                pltpu.VMEM((GROUP, 8, depth, block), F32),
                pltpu.VMEM((GROUP, depth, block, pixels), F32),
                pltpu.VMEM((GROUP, depth, block, pixels), F32),
                pltpu.VMEM((GROUP, depth, 2 * block, pixels), BF16),
                pltpu.VMEM((GROUP, depth, 8, pixels), F32),
                pltpu.VMEM((GROUP, 2 * block, pixels), BF16),
                pltpu.VMEM((GROUP, 8, pixels), F32),
                pltpu.VMEM((GROUP, 16, depth, block), F32),
                pltpu.VMEM((GROUP, 16, depth, block), F32),
            ],
        ),
        out_shape=[
            jax.ShapeDtypeStruct(target.shape, F32),
            jax.ShapeDtypeStruct(arrived.shape, F32),
        ],
        compiler_params=pltpu.CompilerParams(dimension_semantics=("arbitrary",)),
        name="blend",
    )(pairs, tile_place, basis, arrived, target)


def trade(payload):
    return lax.all_to_all(payload, ("gx", "gy"), split_axis=0, concat_axis=0, tiled=True)


def local(splats, moment_one, moment_two, target, tile_place, pairs, fetch):
    devices = lax.axis_size("gx") * lax.axis_size("gy")
    tiles_here = target.shape[0]
    width = 16.0 * TX
    height = 16.0 * (tiles_here * devices // TX)
    order = jnp.asarray(lane_order(splats.shape[2]))

    def project(raw):
        return jnp.dot(derive(raw, width, height), order, precision=lax.Precision.HIGHEST)

    asked = lax.all_to_all(fetch[0], ("gx", "gy"), split_axis=0, concat_axis=0, tiled=True)
    wanted = jnp.maximum(asked, 0)
    own_screen, own_pull = jax.vjp(project, splats)
    payload = own_screen[wanted]
    arrived = trade(payload)
    arrived = arrived.reshape((-1,) + payload.shape[2:])
    image, received_gradients = blend(arrived, target, tile_place, pairs)
    returned = trade(received_gradients.reshape(payload.shape))
    owner_pick = (asked.reshape(-1)[None, :] == jnp.arange(splats.shape[0])[:, None]).astype(
        jnp.float32
    )
    summed = jnp.dot(
        owner_pick, returned.reshape(owner_pick.shape[1], -1), precision=lax.Precision.HIGHEST
    )
    summed = summed.reshape((splats.shape[0],) + returned.shape[2:])
    (splat_grad,) = own_pull(summed)
    first = 0.9 * moment_one + 0.1 * splat_grad
    second_moment = 0.999 * moment_two + 0.001 * splat_grad * splat_grad
    adam_step = first / (jnp.sqrt(second_moment) + 1e-08)
    return (image, splat_grad, adam_step)


def solution(mesh):
    both = ("gx", "gy")
    return jax.shard_map(
        local,
        mesh=mesh,
        in_specs=(
            P(both, None, None),
            P(both, None, None),
            P(both, None, None),
            P(both, None, None),
            P(both),
            P(both, None),
            P(both, None, None),
        ),
        out_specs=(P(both, None, None), P(both, None, None), P(both, None, None)),
        check_vma=False,
    )
```

```python
import functools

import jax
import jax.numpy as jnp
import numpy as np
from jax import lax
from jax.experimental import pallas as pl
from jax.experimental.pallas import tpu as pltpu
from jax.sharding import PartitionSpec as P

TX = 16
SIDE = 16
PIXELS = SIDE * SIDE
LOG2E = 1.4426950408889634
DEAD = -1.0e4
GROUP = 4
F32 = jnp.float32
BF16 = jnp.bfloat16


HARMONIC_ZERO = 0.28209479177387814
HARMONIC_ONE = 0.4886025119029199
HARMONIC_TWO = (
    1.0925484305920792,
    -1.0925484305920792,
    0.31539156525252005,
    -1.0925484305920792,
    0.5462742152960396,
)
HARMONIC_THREE = (
    -0.5900435899266435,
    2.890611442640554,
    -0.4570457994644658,
    0.3731763325901154,
    -0.4570457994644658,
    1.445305721320277,
    -0.5900435899266435,
)


def harmonics(east, north, ahead):
    east_east = east * east
    north_north = north * north
    ahead_ahead = ahead * ahead
    terms = [
        jnp.full_like(east, HARMONIC_ZERO),
        -HARMONIC_ONE * north,
        HARMONIC_ONE * ahead,
        -HARMONIC_ONE * east,
        HARMONIC_TWO[0] * east * north,
        HARMONIC_TWO[1] * north * ahead,
        HARMONIC_TWO[2] * (2.0 * ahead_ahead - east_east - north_north),
        HARMONIC_TWO[3] * east * ahead,
        HARMONIC_TWO[4] * (east_east - north_north),
        HARMONIC_THREE[0] * north * (3.0 * east_east - north_north),
        HARMONIC_THREE[1] * east * north * ahead,
        HARMONIC_THREE[2] * north * (4.0 * ahead_ahead - east_east - north_north),
        HARMONIC_THREE[3] * ahead * (2.0 * ahead_ahead - 3.0 * east_east - 3.0 * north_north),
        HARMONIC_THREE[4] * east * (4.0 * ahead_ahead - east_east - north_north),
        HARMONIC_THREE[5] * ahead * (east_east - north_north),
        HARMONIC_THREE[6] * east * (east_east - 3.0 * north_north),
    ]
    return jnp.stack(terms, axis=1)


def derive(raw, width, height):
    place_x = raw[:, 0]
    place_y = raw[:, 1]
    place_z = raw[:, 2]
    screen_u = width * place_x / place_z + 0.5 * width
    screen_v = width * place_y / place_z + 0.5 * height
    inverse_one = jnp.exp(-2.0 * raw[:, 3])
    inverse_two = jnp.exp(-2.0 * raw[:, 4])
    cosine = jnp.cos(raw[:, 5])
    sine = jnp.sin(raw[:, 5])
    conic_a = cosine * cosine * inverse_one + sine * sine * inverse_two
    conic_b = cosine * sine * (inverse_one - inverse_two)
    conic_c = sine * sine * inverse_one + cosine * cosine * inverse_two
    log_opacity = jax.nn.log_sigmoid(raw[:, 6])
    length = jnp.sqrt(place_x * place_x + place_y * place_y + place_z * place_z)
    basis = harmonics(place_x / length, place_y / length, place_z / length)
    coeffs = raw[:, 7:].reshape(raw.shape[0], 3, 16, raw.shape[2])
    colors = 0.5 + jnp.sum(coeffs * basis[:, None], axis=2)
    head = jnp.stack([screen_u, screen_v, conic_a, conic_b, conic_c, log_opacity], axis=1)
    return jnp.concatenate([head, colors], axis=1)


def pixel_basis():
    j = np.arange(PIXELS)
    x = j % SIDE + 0.5 - SIDE / 2
    y = j // SIDE + 0.5 - SIDE / 2
    rows = np.stack([x * x, x * y, y * y, x, y, np.ones_like(x), 0 * x, 0 * x])
    return np.concatenate([rows, rows, rows, 0 * rows]).astype(np.float32)


def lane_order(block):
    row = np.arange(block)
    splat = (row % 8) * (block // 8) + row // 8
    return (np.arange(block)[:, None] == splat[None, :]).astype(np.float32)


def rounded(x):
    return x.astype(BF16).astype(F32)


def shifted(x, shift):
    return pltpu.roll(x, shift % 8, 0)


def blend_kernel(
    pairs_ref, place_ref, basis_ref, arrived_ref, target_ref, image_ref, grad_ref,
    screen, coef, colour, alphas, weights, halves, products, steps, resid, moments, grads,
):
    step = pl.program_id(0)
    depth = pairs_ref.shape[1]
    block = arrived_ref.shape[2]
    chunks = block // 8
    sub = lax.broadcasted_iota(jnp.int32, (8, PIXELS), 0)
    sub_lane = lax.broadcasted_iota(jnp.int32, (8, block), 0)

    @pl.when(step == 0)
    def _():
        grad_ref[...] = jnp.zeros_like(grad_ref)
        coef[...] = jnp.zeros_like(coef)
        colour[...] = jnp.zeros_like(colour)
        resid[...] = jnp.zeros_like(resid)

    live = []
    centre = []
    deepest = jnp.int32(0)
    for t in range(GROUP):
        row = step * GROUP + t
        tile = place_ref[row]
        count = jnp.int32(0)
        for k in range(depth):
            slot = pairs_ref[row, k]
            count = count + (slot >= 0).astype(jnp.int32)
            screen[t, 0:9, k, :] = arrived_ref[jnp.maximum(slot, 0)]
        live.append(count)
        deepest = jnp.maximum(deepest, count)
        cx = (lax.rem(tile, TX) * SIDE + SIDE // 2).astype(F32)
        cy = (lax.div(tile, TX) * SIDE + SIDE // 2).astype(F32)
        centre.append((cx, cy))
        u = screen[t, 0] - cx
        v = screen[t, 1] - cy
        a, b, c = screen[t, 2], screen[t, 3], screen[t, 4]
        opac = jnp.maximum(screen[t, 5], DEAD)
        lin_x = a * u + b * v
        lin_y = b * u + c * v
        const = opac - 0.5 * (lin_x * u + lin_y * v)
        on = sub_lane < count
        for j, value in enumerate((-0.5 * a, -b, -0.5 * c, lin_x, lin_y, const)):
            coef[t, j] = jnp.where(on, LOG2E * value, DEAD if j == 5 else 0.0)
        for h in range(3):
            colour[t, h] = screen[t, 6 + h]

    basis = basis_ref[...].astype(BF16)
    zero8 = jnp.zeros((8, block), F32)
    zero_row = jnp.zeros((8, PIXELS), F32)

    def forward(k, carry):
        after = []
        for t in range(GROUP):
            trans, total = carry[2 * t], carry[2 * t + 1]
            c = coef[t, :, k, :]
            c1 = rounded(c)
            c2 = rounded(c - c1)
            c3 = c - c1 - c2
            parts = jnp.concatenate([c1, c2, c3, zero8], axis=0).astype(BF16)
            power = lax.dot_general(
                parts, basis, (((0,), (0,)), ((), ())), preferred_element_type=F32
            )
            alpha = jnp.exp2(power)
            alphas[t, k] = alpha
            keep = 1.0 - alpha
            kept = keep[0:8]
            for i in range(1, chunks):
                kept = kept * keep[8 * i : 8 * i + 8]
            products[t, k] = kept
            scan = jnp.where(sub == 0, trans, shifted(kept, 1))
            for d in (1, 2, 4):
                scan = scan * jnp.where(sub < d, 1.0, shifted(scan, d))
            trans = jnp.broadcast_to((scan * kept)[7:8], (8, PIXELS))
            here = scan
            for i in range(0, chunks, 2):
                one = alpha[8 * i : 8 * i + 8] * here
                here = here * keep[8 * i : 8 * i + 8]
                two = alpha[8 * i + 8 : 8 * i + 16] * here
                here = here * keep[8 * i + 8 : 8 * i + 16]
                pair = jnp.concatenate([one, two], axis=0)
                weights[t, k, 8 * i : 8 * i + 16] = pair
                high = pair.astype(BF16)
                halves[t, k, 8 * i : 8 * i + 16] = high
                halves[t, k, block + 8 * i : block + 8 * i + 16] = (
                    pair - high.astype(F32)
                ).astype(BF16)
            hue = colour[t, :, k, :]
            hue1 = rounded(hue)
            hue2 = hue - hue1
            left = jnp.concatenate(
                [
                    jnp.concatenate([hue1, hue1], axis=1),
                    jnp.concatenate([hue2, zero8], axis=1),
                ],
                axis=0,
            ).astype(BF16)
            total = total + jnp.dot(left, halves[t, k], preferred_element_type=F32)
            after += [trans, total]
        return tuple(after)

    start = (jnp.ones((8, PIXELS), F32), jnp.zeros((16, PIXELS), F32)) * GROUP
    done = lax.fori_loop(0, deepest, forward, start)

    slopes = []
    for t in range(GROUP):
        total = done[2 * t + 1]
        image = (total[0:8] + total[8:16])[0:3]
        image_ref[t] = image
        resid[t, 0:3] = (image - target_ref[t]) * (2.0 / 512.0)
        g = resid[t]
        g1 = rounded(g)
        g2 = g - g1
        slopes.append(
            (
                jnp.concatenate([g1, g1, g2, zero_row], axis=0).astype(BF16),
                jnp.concatenate([g1, g2], axis=0).astype(BF16),
            )
        )
    monomials = basis_ref[0:16].astype(BF16)

    def backward(index, carry):
        k = deepest - 1 - index
        after = []
        for t in range(GROUP):
            behind = carry[t]
            g3, g2 = slopes[t]
            hue = colour[t, :, k, :]
            hue1 = rounded(hue)
            hue2 = hue - hue1
            left = jnp.concatenate([hue1, hue2, hue1, zero8], axis=0).astype(BF16)
            slope = lax.dot_general(
                left, g3, (((0,), (0,)), ((), ())), preferred_element_type=F32
            )
            alpha = alphas[t, k]
            keep = 1.0 - alpha
            lit = alpha * slope
            gather = lit[block - 8 : block]
            for i in range(chunks - 2, -1, -1):
                gather = lit[8 * i : 8 * i + 8] + keep[8 * i : 8 * i + 8] * gather
            kept = products[t, k]
            scan = jnp.where(sub == 7, behind, shifted(gather, -1))
            rate = jnp.where(sub == 7, 0.0, shifted(kept, -1))
            for d in (1, 2, 4):
                inside = sub < 8 - d
                scan = scan + rate * jnp.where(inside, shifted(scan, -d), 0.0)
                rate = rate * jnp.where(inside, shifted(rate, -d), 1.0)
            after.append(jnp.broadcast_to((gather + kept * scan)[0:1], (8, PIXELS)))
            here = scan
            for i in range(chunks - 2, -1, -2):
                lo, mid, hi = 8 * i, 8 * i + 8, 8 * i + 16
                two = weights[t, k, mid:hi] * (slope[mid:hi] - here)
                here = lit[mid:hi] + keep[mid:hi] * here
                one = weights[t, k, lo:mid] * (slope[lo:mid] - here)
                here = lit[lo:mid] + keep[lo:mid] * here
                pair = jnp.concatenate([one, two], axis=0)
                high = pair.astype(BF16)
                steps[t, lo:hi] = high
                steps[t, block + lo : block + hi] = (pair - high.astype(F32)).astype(BF16)
            sums = lax.dot_general(
                monomials, steps[t], (((1,), (1,)), ((), ())), preferred_element_type=F32
            )
            moments[t, 0:8, k, :] = sums[0:8, 0:block] + sums[0:8, block:]
            hues = lax.dot_general(
                g2, halves[t, k], (((1,), (1,)), ((), ())), preferred_element_type=F32
            )
            moments[t, 8:16, k, :] = hues[0:8, 0:block] + hues[0:8, block:] + hues[8:16, 0:block]
        return tuple(after)

    lax.fori_loop(0, deepest, backward, (jnp.zeros((8, PIXELS), F32),) * GROUP)

    for t in range(GROUP):
        row = step * GROUP + t
        cx, cy = centre[t]
        u = screen[t, 0] - cx
        v = screen[t, 1] - cy
        a, b, c = screen[t, 2], screen[t, 3], screen[t, 4]
        mxx, mxy, myy = moments[t, 0], moments[t, 1], moments[t, 2]
        mx, my, m = moments[t, 3], moments[t, 4], moments[t, 5]
        off_x = mx - u * m
        off_y = my - v * m
        grads[t, 0] = a * off_x + b * off_y
        grads[t, 1] = b * off_x + c * off_y
        grads[t, 2] = -0.5 * (mxx - u * (mx + off_x))
        grads[t, 3] = -(mxy - u * my - v * off_x)
        grads[t, 4] = -0.5 * (myy - v * (my + off_y))
        grads[t, 5] = m
        for h in range(3):
            grads[t, 6 + h] = moments[t, 8 + h]
        for k in range(depth):

            @pl.when(k < live[t])
            def _():
                slot = pairs_ref[row, k]
                grad_ref[slot] = grad_ref[slot] + grads[t, 0:9, k, :]


def blend(arrived, target, tile_place, pairs):
    tiles, channels, pixels = target.shape
    depth = pairs.shape[1]
    slots, rows, block = arrived.shape
    basis = jnp.asarray(pixel_basis())
    whole = lambda s, *_: (0, 0, 0)
    return pl.pallas_call(
        blend_kernel,
        grid_spec=pltpu.PrefetchScalarGridSpec(
            num_scalar_prefetch=2,
            grid=(tiles // GROUP,),
            in_specs=[
                pl.BlockSpec(basis.shape, lambda s, *_: (0, 0)),
                pl.BlockSpec(arrived.shape, whole),
                pl.BlockSpec((GROUP, channels, pixels), lambda s, *_: (s, 0, 0)),
            ],
            out_specs=[
                pl.BlockSpec((GROUP, channels, pixels), lambda s, *_: (s, 0, 0)),
                pl.BlockSpec(arrived.shape, whole),
            ],
            scratch_shapes=[
                pltpu.VMEM((GROUP, 16, depth, block), F32),
                pltpu.VMEM((GROUP, 8, depth, block), F32),
                pltpu.VMEM((GROUP, 8, depth, block), F32),
                pltpu.VMEM((GROUP, depth, block, pixels), F32),
                pltpu.VMEM((GROUP, depth, block, pixels), F32),
                pltpu.VMEM((GROUP, depth, 2 * block, pixels), BF16),
                pltpu.VMEM((GROUP, depth, 8, pixels), F32),
                pltpu.VMEM((GROUP, 2 * block, pixels), BF16),
                pltpu.VMEM((GROUP, 8, pixels), F32),
                pltpu.VMEM((GROUP, 16, depth, block), F32),
                pltpu.VMEM((GROUP, 16, depth, block), F32),
            ],
        ),
        out_shape=[
            jax.ShapeDtypeStruct(target.shape, F32),
            jax.ShapeDtypeStruct(arrived.shape, F32),
        ],
        compiler_params=pltpu.CompilerParams(dimension_semantics=("arbitrary",)),
        name="blend",
    )(pairs, tile_place, basis, arrived, target)


def trade(payload):
    return lax.all_to_all(payload, ("gx", "gy"), split_axis=0, concat_axis=0, tiled=True)


def local(splats, moment_one, moment_two, target, tile_place, pairs, fetch):
    devices = lax.axis_size("gx") * lax.axis_size("gy")
    tiles_here = target.shape[0]
    width = 16.0 * TX
    height = 16.0 * (tiles_here * devices // TX)
    order = jnp.asarray(lane_order(splats.shape[2]))

    def project(raw):
        return jnp.dot(derive(raw, width, height), order, precision=lax.Precision.HIGHEST)

    asked = lax.all_to_all(fetch[0], ("gx", "gy"), split_axis=0, concat_axis=0, tiled=True)
    wanted = jnp.maximum(asked, 0)
    own_screen, own_pull = jax.vjp(project, splats)
    payload = own_screen[wanted]
    arrived = trade(payload)
    arrived = arrived.reshape((-1,) + payload.shape[2:])
    image, received_gradients = blend(arrived, target, tile_place, pairs)
    returned = trade(received_gradients.reshape(payload.shape))
    owner_pick = (asked.reshape(-1)[None, :] == jnp.arange(splats.shape[0])[:, None]).astype(
        jnp.float32
    )
    summed = jnp.dot(
        owner_pick, returned.reshape(owner_pick.shape[1], -1), precision=lax.Precision.HIGHEST
    )
    summed = summed.reshape((splats.shape[0],) + returned.shape[2:])
    (splat_grad,) = own_pull(summed)
    first = 0.9 * moment_one + 0.1 * splat_grad
    second_moment = 0.999 * moment_two + 0.001 * splat_grad * splat_grad
    adam_step = first / (jnp.sqrt(second_moment) + 1e-08)
    return (image, splat_grad, adam_step)


def solution(mesh):
    both = ("gx", "gy")
    return jax.shard_map(
        local,
        mesh=mesh,
        in_specs=(
            P(both, None, None),
            P(both, None, None),
            P(both, None, None),
            P(both, None, None),
            P(both),
            P(both, None),
            P(both, None, None),
        ),
        out_specs=(P(both, None, None), P(both, None, None), P(both, None, None)),
        check_vma=False,
    )
```

```python
import functools

import jax
import jax.numpy as jnp
import numpy as np
from jax import lax
from jax.experimental import pallas as pl
from jax.experimental.pallas import tpu as pltpu
from jax.sharding import PartitionSpec as P

TX = 16
SIDE = 16
PIXELS = SIDE * SIDE
LOG2E = 1.4426950408889634
DEAD = -1.0e4
GROUP = 4
F32 = jnp.float32
BF16 = jnp.bfloat16


HARMONIC_ZERO = 0.28209479177387814
HARMONIC_ONE = 0.4886025119029199
HARMONIC_TWO = (
    1.0925484305920792,
    -1.0925484305920792,
    0.31539156525252005,
    -1.0925484305920792,
    0.5462742152960396,
)
HARMONIC_THREE = (
    -0.5900435899266435,
    2.890611442640554,
    -0.4570457994644658,
    0.3731763325901154,
    -0.4570457994644658,
    1.445305721320277,
    -0.5900435899266435,
)


def harmonics(east, north, ahead):
    east_east = east * east
    north_north = north * north
    ahead_ahead = ahead * ahead
    terms = [
        jnp.full_like(east, HARMONIC_ZERO),
        -HARMONIC_ONE * north,
        HARMONIC_ONE * ahead,
        -HARMONIC_ONE * east,
        HARMONIC_TWO[0] * east * north,
        HARMONIC_TWO[1] * north * ahead,
        HARMONIC_TWO[2] * (2.0 * ahead_ahead - east_east - north_north),
        HARMONIC_TWO[3] * east * ahead,
        HARMONIC_TWO[4] * (east_east - north_north),
        HARMONIC_THREE[0] * north * (3.0 * east_east - north_north),
        HARMONIC_THREE[1] * east * north * ahead,
        HARMONIC_THREE[2] * north * (4.0 * ahead_ahead - east_east - north_north),
        HARMONIC_THREE[3] * ahead * (2.0 * ahead_ahead - 3.0 * east_east - 3.0 * north_north),
        HARMONIC_THREE[4] * east * (4.0 * ahead_ahead - east_east - north_north),
        HARMONIC_THREE[5] * ahead * (east_east - north_north),
        HARMONIC_THREE[6] * east * (east_east - 3.0 * north_north),
    ]
    return jnp.stack(terms, axis=1)


def derive(raw, width, height):
    place_x = raw[:, 0]
    place_y = raw[:, 1]
    place_z = raw[:, 2]
    screen_u = width * place_x / place_z + 0.5 * width
    screen_v = width * place_y / place_z + 0.5 * height
    inverse_one = jnp.exp(-2.0 * raw[:, 3])
    inverse_two = jnp.exp(-2.0 * raw[:, 4])
    cosine = jnp.cos(raw[:, 5])
    sine = jnp.sin(raw[:, 5])
    conic_a = cosine * cosine * inverse_one + sine * sine * inverse_two
    conic_b = cosine * sine * (inverse_one - inverse_two)
    conic_c = sine * sine * inverse_one + cosine * cosine * inverse_two
    log_opacity = jax.nn.log_sigmoid(raw[:, 6])
    length = jnp.sqrt(place_x * place_x + place_y * place_y + place_z * place_z)
    basis = harmonics(place_x / length, place_y / length, place_z / length)
    coeffs = raw[:, 7:].reshape(raw.shape[0], 3, 16, raw.shape[2])
    colors = 0.5 + jnp.sum(coeffs * basis[:, None], axis=2)
    head = jnp.stack([screen_u, screen_v, conic_a, conic_b, conic_c, log_opacity], axis=1)
    return jnp.concatenate([head, colors], axis=1)


def pixel_basis():
    j = np.arange(PIXELS)
    x = j % SIDE + 0.5 - SIDE / 2
    y = j // SIDE + 0.5 - SIDE / 2
    rows = np.stack([x * x, x * y, y * y, x, y, np.ones_like(x), 0 * x, 0 * x])
    return np.concatenate([rows, rows, rows, 0 * rows]).astype(np.float32)


def lane_order(block):
    row = np.arange(block)
    splat = (row % 8) * (block // 8) + row // 8
    return (np.arange(block)[:, None] == splat[None, :]).astype(np.float32)


def rounded(x):
    return x.astype(BF16).astype(F32)


def shifted(x, shift):
    return pltpu.roll(x, shift % 8, 0)


def blend_kernel(
    pairs_ref, place_ref, basis_ref, arrived_ref, target_ref, image_ref, grad_ref,
    screen, coef, colour, alphas, weights, halves, products, steps, resid, moments, grads,
):
    step = pl.program_id(0)
    depth = pairs_ref.shape[1]
    block = arrived_ref.shape[2]
    chunks = block // 8
    sub = lax.broadcasted_iota(jnp.int32, (8, PIXELS), 0)
    sub_lane = lax.broadcasted_iota(jnp.int32, (8, block), 0)

    @pl.when(step == 0)
    def _():
        grad_ref[...] = jnp.zeros_like(grad_ref)
        coef[...] = jnp.zeros_like(coef)
        colour[...] = jnp.zeros_like(colour)
        resid[...] = jnp.zeros_like(resid)

    live = []
    centre = []
    deepest = jnp.int32(0)
    for t in range(GROUP):
        row = step * GROUP + t
        tile = place_ref[row]
        count = jnp.int32(0)
        for k in range(depth):
            slot = pairs_ref[row, k]
            count = count + (slot >= 0).astype(jnp.int32)
            screen[t, 0:9, k, :] = arrived_ref[jnp.maximum(slot, 0)]
        live.append(count)
        deepest = jnp.maximum(deepest, count)
        cx = (lax.rem(tile, TX) * SIDE + SIDE // 2).astype(F32)
        cy = (lax.div(tile, TX) * SIDE + SIDE // 2).astype(F32)
        centre.append((cx, cy))
        u = screen[t, 0] - cx
        v = screen[t, 1] - cy
        a, b, c = screen[t, 2], screen[t, 3], screen[t, 4]
        opac = jnp.maximum(screen[t, 5], DEAD)
        lin_x = a * u + b * v
        lin_y = b * u + c * v
        const = opac - 0.5 * (lin_x * u + lin_y * v)
        on = sub_lane < count
        for j, value in enumerate((-0.5 * a, -b, -0.5 * c, lin_x, lin_y, const)):
            coef[t, j] = jnp.where(on, LOG2E * value, DEAD if j == 5 else 0.0)
        for h in range(3):
            colour[t, h] = screen[t, 6 + h]

    basis = basis_ref[...].astype(BF16)
    zero8 = jnp.zeros((8, block), F32)
    zero_row = jnp.zeros((8, PIXELS), F32)

    def forward(k, carry):
        after = []
        for t in range(GROUP):
            trans, total = carry[2 * t], carry[2 * t + 1]
            c = coef[t, :, k, :]
            c1 = rounded(c)
            c2 = rounded(c - c1)
            c3 = c - c1 - c2
            parts = jnp.concatenate([c1, c2, c3, zero8], axis=0).astype(BF16)
            power = lax.dot_general(
                parts, basis, (((0,), (0,)), ((), ())), preferred_element_type=F32
            )
            alpha = jnp.exp2(power)
            alphas[t, k] = alpha
            keep = 1.0 - alpha
            kept = keep[0:8]
            for i in range(1, chunks):
                kept = kept * keep[8 * i : 8 * i + 8]
            products[t, k] = kept
            scan = jnp.where(sub == 0, trans, shifted(kept, 1))
            for d in (1, 2, 4):
                scan = scan * jnp.where(sub < d, 1.0, shifted(scan, d))
            trans = jnp.broadcast_to((scan * kept)[7:8], (8, PIXELS))
            here = scan
            for i in range(0, chunks, 2):
                one = alpha[8 * i : 8 * i + 8] * here
                here = here * keep[8 * i : 8 * i + 8]
                two = alpha[8 * i + 8 : 8 * i + 16] * here
                here = here * keep[8 * i + 8 : 8 * i + 16]
                pair = jnp.concatenate([one, two], axis=0)
                weights[t, k, 8 * i : 8 * i + 16] = pair
                high = pair.astype(BF16)
                halves[t, k, 8 * i : 8 * i + 16] = high
                halves[t, k, block + 8 * i : block + 8 * i + 16] = (
                    pair - high.astype(F32)
                ).astype(BF16)
            hue = colour[t, :, k, :]
            hue1 = rounded(hue)
            hue2 = hue - hue1
            left = jnp.concatenate(
                [
                    jnp.concatenate([hue1, hue1], axis=1),
                    jnp.concatenate([hue2, zero8], axis=1),
                ],
                axis=0,
            ).astype(BF16)
            total = total + jnp.dot(left, halves[t, k], preferred_element_type=F32)
            after += [trans, total]
        return tuple(after)

    start = (jnp.ones((8, PIXELS), F32), jnp.zeros((16, PIXELS), F32)) * GROUP
    done = lax.fori_loop(0, deepest, forward, start)

    slopes = []
    for t in range(GROUP):
        total = done[2 * t + 1]
        image = (total[0:8] + total[8:16])[0:3]
        image_ref[t] = image
        resid[t, 0:3] = (image - target_ref[t]) * (2.0 / 512.0)
        g = resid[t]
        g1 = rounded(g)
        g2 = g - g1
        slopes.append(
            (
                jnp.concatenate([g1, g1, g2, zero_row], axis=0).astype(BF16),
                jnp.concatenate([g1, g2], axis=0).astype(BF16),
            )
        )
    monomials = basis_ref[0:16].astype(BF16)

    def backward(index, carry):
        k = deepest - 1 - index
        after = []
        for t in range(GROUP):
            behind = carry[t]
            g3, g2 = slopes[t]
            hue = colour[t, :, k, :]
            hue1 = rounded(hue)
            hue2 = hue - hue1
            left = jnp.concatenate([hue1, hue2, hue1, zero8], axis=0).astype(BF16)
            slope = lax.dot_general(
                left, g3, (((0,), (0,)), ((), ())), preferred_element_type=F32
            )
            alpha = alphas[t, k]
            keep = 1.0 - alpha
            lit = alpha * slope
            gather = lit[block - 8 : block]
            for i in range(chunks - 2, -1, -1):
                gather = lit[8 * i : 8 * i + 8] + keep[8 * i : 8 * i + 8] * gather
            kept = products[t, k]
            scan = jnp.where(sub == 7, behind, shifted(gather, -1))
            rate = jnp.where(sub == 7, 0.0, shifted(kept, -1))
            for d in (1, 2, 4):
                inside = sub < 8 - d
                scan = scan + rate * jnp.where(inside, shifted(scan, -d), 0.0)
                rate = rate * jnp.where(inside, shifted(rate, -d), 1.0)
            after.append(jnp.broadcast_to((gather + kept * scan)[0:1], (8, PIXELS)))
            here = scan
            for i in range(chunks - 2, -1, -2):
                lo, mid, hi = 8 * i, 8 * i + 8, 8 * i + 16
                two = weights[t, k, mid:hi] * (slope[mid:hi] - here)
                here = lit[mid:hi] + keep[mid:hi] * here
                one = weights[t, k, lo:mid] * (slope[lo:mid] - here)
                here = lit[lo:mid] + keep[lo:mid] * here
                pair = jnp.concatenate([one, two], axis=0)
                high = pair.astype(BF16)
                steps[t, lo:hi] = high
                steps[t, block + lo : block + hi] = (pair - high.astype(F32)).astype(BF16)
            sums = lax.dot_general(
                monomials, steps[t], (((1,), (1,)), ((), ())), preferred_element_type=F32
            )
            moments[t, 0:8, k, :] = sums[0:8, 0:block] + sums[0:8, block:]
            hues = lax.dot_general(
                g2, halves[t, k], (((1,), (1,)), ((), ())), preferred_element_type=F32
            )
            moments[t, 8:16, k, :] = hues[0:8, 0:block] + hues[0:8, block:] + hues[8:16, 0:block]
        return tuple(after)

    lax.fori_loop(0, deepest, backward, (jnp.zeros((8, PIXELS), F32),) * GROUP)

    for t in range(GROUP):
        row = step * GROUP + t
        cx, cy = centre[t]
        u = screen[t, 0] - cx
        v = screen[t, 1] - cy
        a, b, c = screen[t, 2], screen[t, 3], screen[t, 4]
        mxx, mxy, myy = moments[t, 0], moments[t, 1], moments[t, 2]
        mx, my, m = moments[t, 3], moments[t, 4], moments[t, 5]
        off_x = mx - u * m
        off_y = my - v * m
        grads[t, 0] = a * off_x + b * off_y
        grads[t, 1] = b * off_x + c * off_y
        grads[t, 2] = -0.5 * (mxx - u * (mx + off_x))
        grads[t, 3] = -(mxy - u * my - v * off_x)
        grads[t, 4] = -0.5 * (myy - v * (my + off_y))
        grads[t, 5] = m
        for h in range(3):
            grads[t, 6 + h] = moments[t, 8 + h]
        for k in range(depth):

            @pl.when(k < live[t])
            def _():
                slot = pairs_ref[row, k]
                grad_ref[slot] = grad_ref[slot] + grads[t, 0:9, k, :]


def blend(arrived, target, tile_place, pairs):
    tiles, channels, pixels = target.shape
    depth = pairs.shape[1]
    slots, rows, block = arrived.shape
    basis = jnp.asarray(pixel_basis())
    whole = lambda s, *_: (0, 0, 0)
    return pl.pallas_call(
        blend_kernel,
        grid_spec=pltpu.PrefetchScalarGridSpec(
            num_scalar_prefetch=2,
            grid=(tiles // GROUP,),
            in_specs=[
                pl.BlockSpec(basis.shape, lambda s, *_: (0, 0)),
                pl.BlockSpec(arrived.shape, whole),
                pl.BlockSpec((GROUP, channels, pixels), lambda s, *_: (s, 0, 0)),
            ],
            out_specs=[
                pl.BlockSpec((GROUP, channels, pixels), lambda s, *_: (s, 0, 0)),
                pl.BlockSpec(arrived.shape, whole),
            ],
            scratch_shapes=[
                pltpu.VMEM((GROUP, 16, depth, block), F32),
                pltpu.VMEM((GROUP, 8, depth, block), F32),
                pltpu.VMEM((GROUP, 8, depth, block), F32),
                pltpu.VMEM((GROUP, depth, block, pixels), F32),
                pltpu.VMEM((GROUP, depth, block, pixels), F32),
                pltpu.VMEM((GROUP, depth, 2 * block, pixels), BF16),
                pltpu.VMEM((GROUP, depth, 8, pixels), F32),
                pltpu.VMEM((GROUP, 2 * block, pixels), BF16),
                pltpu.VMEM((GROUP, 8, pixels), F32),
                pltpu.VMEM((GROUP, 16, depth, block), F32),
                pltpu.VMEM((GROUP, 16, depth, block), F32),
            ],
        ),
        out_shape=[
            jax.ShapeDtypeStruct(target.shape, F32),
            jax.ShapeDtypeStruct(arrived.shape, F32),
        ],
        compiler_params=pltpu.CompilerParams(dimension_semantics=("arbitrary",)),
        name="blend",
    )(pairs, tile_place, basis, arrived, target)


def trade_kernel(sizes, send, recv, send_sem, recv_sem, own_sem):
    inner = sizes[1]
    total = sizes[0] * inner
    me = lax.axis_index("gx") * inner + lax.axis_index("gy")

    def peer(step):
        other = lax.rem(me + step, total)
        return other, {"gx": lax.div(other, inner), "gy": lax.rem(other, inner)}

    barrier = pltpu.get_barrier_semaphore()

    @pl.loop(1, total)
    def _(step):
        pl.semaphore_signal(
            barrier, inc=1, device_id=peer(step)[1], device_id_type=pl.DeviceIdType.MESH
        )

    own = pltpu.make_async_copy(send.at[me], recv.at[me], own_sem)
    own.start()
    pl.semaphore_wait(barrier, total - 1)

    def copy(step):
        other, place = peer(step)
        return pltpu.make_async_remote_copy(
            src_ref=send.at[other],
            dst_ref=recv.at[me],
            send_sem=send_sem.at[step],
            recv_sem=recv_sem.at[step],
            device_id=place,
            device_id_type=pl.DeviceIdType.MESH,
        )

    @pl.loop(1, total)
    def _(step):
        copy(step).start()

    own.wait()

    @pl.loop(1, total)
    def _(step):
        copy(step).wait()


def trade(payload, name, collective_id):
    sizes = (lax.axis_size("gx"), lax.axis_size("gy"))
    total = sizes[0] * sizes[1]
    return pl.pallas_call(
        functools.partial(trade_kernel, sizes),
        out_shape=jax.ShapeDtypeStruct(payload.shape, payload.dtype),
        in_specs=[pl.BlockSpec(memory_space=pltpu.VMEM)],
        out_specs=pl.BlockSpec(memory_space=pltpu.VMEM),
        scratch_shapes=[
            pltpu.SemaphoreType.DMA((total,)),
            pltpu.SemaphoreType.DMA((total,)),
            pltpu.SemaphoreType.DMA,
        ],
        compiler_params=pltpu.CompilerParams(
            collective_id=collective_id, has_side_effects=True
        ),
        name=name,
    )(payload)


def local(splats, moment_one, moment_two, target, tile_place, pairs, fetch):
    devices = lax.axis_size("gx") * lax.axis_size("gy")
    tiles_here = target.shape[0]
    width = 16.0 * TX
    height = 16.0 * (tiles_here * devices // TX)
    order = jnp.asarray(lane_order(splats.shape[2]))

    def project(raw):
        return jnp.dot(derive(raw, width, height), order, precision=lax.Precision.HIGHEST)

    request = jnp.zeros((devices, 8, 128), jnp.int32)
    request = request.at[:, 0, : fetch.shape[2]].set(fetch[0])
    asked = trade(request, "ask", 0)[:, 0, : fetch.shape[2]]
    wanted = jnp.maximum(asked, 0)
    own_screen, own_pull = jax.vjp(project, splats)
    payload = own_screen[wanted]
    arrived = trade(payload, "send", 1)
    arrived = arrived.reshape((-1,) + payload.shape[2:])
    image, received_gradients = blend(arrived, target, tile_place, pairs)
    returned = trade(received_gradients.reshape(payload.shape), "give", 2)
    owner_pick = (asked.reshape(-1)[None, :] == jnp.arange(splats.shape[0])[:, None]).astype(
        jnp.float32
    )
    summed = jnp.dot(
        owner_pick, returned.reshape(owner_pick.shape[1], -1), precision=lax.Precision.HIGHEST
    )
    summed = summed.reshape((splats.shape[0],) + returned.shape[2:])
    (splat_grad,) = own_pull(summed)
    first = 0.9 * moment_one + 0.1 * splat_grad
    second_moment = 0.999 * moment_two + 0.001 * splat_grad * splat_grad
    adam_step = first / (jnp.sqrt(second_moment) + 1e-08)
    return (image, splat_grad, adam_step)


def solution(mesh):
    both = ("gx", "gy")
    return jax.shard_map(
        local,
        mesh=mesh,
        in_specs=(
            P(both, None, None),
            P(both, None, None),
            P(both, None, None),
            P(both, None, None),
            P(both),
            P(both, None),
            P(both, None, None),
        ),
        out_specs=(P(both, None, None), P(both, None, None), P(both, None, None)),
        check_vma=False,
    )
```
